128 devices in a mesh: gx: 8 (over x_lo, y), gy: 16 (over x_hi, z, core).
Axes of the slice: x: 4 (x_hi: 2, x_lo: 2; x = x_hi * 2 + x_lo), y: 4, z: 4, core: 2. Of those that a mesh axis runs over, the one named last changes fastest.
Arguments:
- density: float32 [64, 64, 128], P('gx', 'gy'), may hold values from -5 to 5
- susceptibility: float32 [64, 64, 128], P('gx', 'gy'), may hold values from -5 to 5
- station_cell: int32 [2, 2048], P(None, 'gx'), may hold values from 0 to 4095
- station_line: int32 [2, 2048], P(None, 'gx'), may hold values from 0 to 255, as said below
- observed: float32 [2, 2048], P(None, 'gx'), may hold values from -3 to 3
- data_weight: float32 [2, 2048], P(None, 'gx'), may hold values from 0.5 to 2
- trial_steps: float32 [8], replicated, may hold values from 0.05 to 0.5
Outputs:
- data_gradient: float32 [2, 64, 64, 128], P(None, 'gx', 'gy')
- cross_force: float32 [2, 64, 64, 128], P(None, 'gx', 'gy')
- weighted_residual: float32 [2, 2048], P(None, 'gx')
- trial_values: float32 [8], replicated
The draws below stay inside these ranges and needn't reach their ends.
Inputs may be any that keep to these rules, and one draw needn't show every extreme that they name: `station_line`: one or more survey lines hold no station of either field.
All inputs are finite; a program needn't handle non-finite values. Where the reference program divides by a largest or mean magnitude, that divisor is 1e-20 or more.
Results may differ from the reference program's by a relative error of at most 0.0003.
Values sent between devices are 32-bit elements; how exact they have to be, the bound alone decides.
A program may use at most 64 MiB of HBM per device.

```python
import math
import jax
import jax.numpy as jnp
from jax import lax

NZ = 128
LINES = 256
TRIALS = 8
NX = 64
NY = 64
STATIONS = 2048


def draw_density(key, part):
    return jnp.clip(jax.random.normal(key, (NX, NY, NZ), jnp.float32), -5.0, 5.0)


def draw_susceptibility(key, part):
    inner = jax.random.fold_in(key, 7)
    return jnp.clip(jax.random.normal(inner, (NX, NY, NZ), jnp.float32), -5.0, 5.0)


def draw_station_line(key, part):
    table_key = jax.random.fold_in(key, 11)
    pick_key = jax.random.fold_in(key, 12)
    missing_key = jax.random.fold_in(key, 13)
    table = jax.random.randint(table_key, (LINES,), 0, LINES, jnp.int32)
    missing = jax.random.randint(missing_key, (), 0, LINES, jnp.int32)
    table = jnp.where(table == missing, (table + 1) % LINES, table)
    picks = jax.random.randint(pick_key, (2, STATIONS), 0, LINES, jnp.int32)
    return table[picks]


def with_ends(result, key, least, high):
    longest = result.shape.index(max(result.shape))
    spots = []
    for shift in (0, 1):
        where = [jax.random.randint(jax.random.fold_in(key, axis), (), 0, length) for axis, length in enumerate(result.shape)]
        where[longest] = (where[longest] + shift) % result.shape[longest]
        spots.append(tuple(where))
    return result.at[spots[0]].set(least).at[spots[1]].set(high)


def steps_of(key, dims, shards, least, largest):
    loudness = 1.0
    for dim, shards_of in shards:
        heights = jax.random.uniform(jax.random.fold_in(jax.random.fold_in(key, 6), dim), (shards_of,), jnp.float32, least / len(shards), largest / len(shards))
        loudness = loudness * jnp.repeat(jnp.exp(heights), dims[dim] // shards_of).reshape((-1,) + (1,) * (len(dims) - 1 - dim))
    return loudness


def gaussian(stream_key, shape, width, limit, split=(), kind=jnp.bfloat16):
    entries = jax.random.normal(stream_key, shape, jnp.float32) * width
    if len(split) > 0:
        entries = steps_of(stream_key, shape, split, -0.22, 0.18) * entries
    return jnp.clip(entries, min=-limit, max=limit).astype(kind)


def setup_inputs(seed: int = 0) -> dict:
    streams_of = jax.random.split(jax.random.key(seed), 8)
    return {
        "density": draw_density(jax.random.fold_in(streams_of[7], 71), 0),
        "susceptibility": draw_susceptibility(jax.random.fold_in(streams_of[7], 71), 0),
        "station_cell": with_ends(jax.random.randint(streams_of[2], (2, STATIONS), 0, NX * NY), jax.random.fold_in(streams_of[2], 1), 0, (NX * NY) - 1).astype(jnp.int32),
        "station_line": draw_station_line(jax.random.fold_in(streams_of[7], 71), 0),
        "observed": gaussian(streams_of[4], (2, STATIONS), 0.5, 3.0, ((1, 8),), jnp.float32),
        "data_weight": jnp.clip(jnp.exp(math.log(2.0) - 1.3862944 * jax.random.uniform(streams_of[5], (2, STATIONS), jnp.float32) ** steps_of(streams_of[5], (2, STATIONS), ((1, 8),), -0.2, 0.2)), 0.5, 2.0),
        "trial_steps": jnp.clip(jnp.exp(jax.random.uniform(streams_of[6], (TRIALS,), jnp.float32, math.log(0.05), math.log(0.5))), 0.05, 0.5),
    }


cell_depth = 2.0
lift = 1.0
coupling_scale = 0.05
highest = lax.Precision.HIGHEST

def kernel_tile(field, station_x, station_y, cell_x, cell_y, depth):
    gap_x = station_x[:, None] - cell_x[None, :]
    gap_y = station_y[:, None] - cell_y[None, :]
    depth_row = depth[None, :]
    radius_sq = gap_x * gap_x + gap_y * gap_y + depth_row * depth_row
    inverse = lax.rsqrt(radius_sq)
    cube = inverse * inverse * inverse
    if field == 0:
        return depth_row * cube
    return (3.0 * depth_row * depth_row - radius_sq) * cube * inverse * inverse

def cell_coords(start, count):
    position = start + jnp.arange(count, dtype=jnp.int32)
    cell_x = (position // (NY * NZ)).astype(jnp.float32)
    cell_y = (position // NZ % NY).astype(jnp.float32)
    depth = ((position % NZ).astype(jnp.float32) + 0.5) * cell_depth + lift
    return (cell_x, cell_y, depth)

def forward_all(models, station_x, station_y):
    flat = models.reshape(2, -1)
    cells = flat.shape[1]
    block = math.gcd(cells, 8192)

    def turn(index, total):
        start = (index * block).astype(jnp.int32)
        cell_x, cell_y, depth = cell_coords(start, block)
        piece = lax.dynamic_slice_in_dim(flat, start, block, 1)
        rows = [jnp.dot(kernel_tile(field, station_x[field], station_y[field], cell_x, cell_y, depth), piece[field], precision=highest) for field in range(2)]
        return total + jnp.stack(rows)
    return lax.fori_loop(0, cells // block, turn, jnp.zeros((2, station_x.shape[1]), jnp.float32))

def adjoint_all(source, station_x, station_y):
    cells = NX * NY * NZ
    block = math.gcd(cells, 8192)

    def turn(index):
        start = (index * block).astype(jnp.int32)
        cell_x, cell_y, depth = cell_coords(start, block)
        rows = [jnp.dot(source[field], kernel_tile(field, station_x[field], station_y[field], cell_x, cell_y, depth), precision=highest) for field in range(2)]
        return jnp.stack(rows)
    parts = lax.map(turn, jnp.arange(cells // block, dtype=jnp.int32))
    return jnp.swapaxes(parts, 0, 1).reshape(2, NX, NY, NZ)

def forward_diffs(field):
    along_x = jnp.concatenate([field[1:] - field[:-1], jnp.zeros_like(field[:1])], axis=0)
    along_y = jnp.concatenate([field[:, 1:] - field[:, :-1], jnp.zeros_like(field[:, :1])], axis=1)
    along_z = jnp.concatenate([field[:, :, 1:] - field[:, :, :-1], jnp.zeros_like(field[:, :, :1])], axis=2)
    return (along_x, along_y, along_z)

def cross_energy(models):
    first_x, first_y, first_z = forward_diffs(models[0])
    second_x, second_y, second_z = forward_diffs(models[1])
    part_one = first_y * second_z - first_z * second_y
    part_two = first_z * second_x - first_x * second_z
    part_three = first_x * second_y - first_y * second_x
    return 0.5 * jnp.sum(part_one * part_one + part_two * part_two + part_three * part_three)

def level(values, lines):

    def one(value_row, line_row):
        sums = jax.ops.segment_sum(value_row, line_row, LINES)
        counts = jax.ops.segment_sum(jnp.ones_like(value_row), line_row, LINES)
        means = sums / jnp.maximum(counts, 1.0)
        return value_row - means[line_row]
    return jax.vmap(one)(values, lines)

def reference(density, susceptibility, station_cell, station_line, observed, data_weight, trial_steps):
    models = jnp.stack([density, susceptibility])
    station_x = (station_cell // NY).astype(jnp.float32)
    station_y = (station_cell % NY).astype(jnp.float32)
    total_stations = station_cell.shape[1]
    predicted = forward_all(models, station_x, station_y)
    residual = level(predicted - observed, station_line)
    weighted_residual = data_weight * residual
    source = level(data_weight * weighted_residual, station_line)
    data_gradient = adjoint_all(source, station_x, station_y)
    cross_force = jax.grad(cross_energy)(models)
    coupling = coupling_scale * total_stations / (NX * NY * NZ)
    gradient = data_gradient + coupling * cross_force
    peak = jnp.max(jnp.abs(gradient)) + 1e-06
    direction = gradient / peak
    image = forward_all(direction, station_x, station_y)
    change = level(image, station_line)
    values = []
    for trial in range(TRIALS):
        step = trial_steps[trial]
        moved = data_weight * (residual - step * change)
        values.append((0.5 * jnp.sum(moved * moved) + coupling * cross_energy(models - step * direction)) / (2 * total_stations))
    return (data_gradient, cross_force, weighted_residual, jnp.stack(values))
```

```python
import jax
import jax.numpy as jnp
from jax import lax
from jax.experimental import pallas as pl
from jax.experimental.pallas import tpu as pltpu
from jax.sharding import Mesh
from jax.sharding import PartitionSpec as P

AXES = ("xl", "y", "xh", "z", "c")
GX = ("xl", "y")
GY = ("xh", "z", "c")

NX = 64
NY = 64
NZ = 128
STATIONS = 2048
LINES = 256
TRIALS = 8
SIDE = 8
PAD = 8
US = NX + PAD
LANES = 128
cell_depth = 2.0
lift = 1.0
coupling = 0.05 * STATIONS / (NX * NY * NZ)

f32 = jnp.float32
bf16 = jnp.bfloat16
MESH = pl.DeviceIdType.MESH


def split(value):
    high = value.astype(bf16)
    low = (value - high.astype(f32)).astype(bf16)
    return high, low


def rounded(value):
    high = value.astype(bf16).astype(f32)
    return high, value - high


def dot(a, b):
    return jnp.dot(a, b, preferred_element_type=f32)


def dot_nt(a, b):
    return lax.dot_general(a, b, (((1,), (1,)), ((), ())), preferred_element_type=f32)


def iota(shape, axis):
    return lax.broadcasted_iota(jnp.int32, shape, axis)


def kernel(
    den, sus, cell, line, obs, wgt, steps,
    dg_out, cf_out, wr_out, tv_out,
    blk, cell_v, line_v, obs_v, wgt_v, st, rowv, tt, ar1, ar2, ar3,
    ohx, ohy, ohl, xlo, xhi, ylo_s, yhi_s, ylo, yhi, big,
    e_hi, e_lo, x_hi, x_lo, sgp, dgb, cfb, cfo, dgo, wr_all, wrx, wro, fin, tvo, inv_cnt,
    load_sem, out_sem, pair_send, pair_recv, st_send, st_recv,
    a1_send, a1_recv, a2_send, a2_recv, a3_send, a3_recv, halo_send, halo_recv,
):
    xl, y, xh, z, c = (lax.axis_index(a) for a in AXES)
    bx = xl * 4 + y
    by = xh * 4 + z
    px = xh * 2 + xl
    i0 = bx * SIDE
    j0 = by * SIDE
    pending = []

    def remote(src, dst, send, recv, device):
        return pltpu.make_async_remote_copy(
            src_ref=src, dst_ref=dst, send_sem=send, recv_sem=recv, device_id=device, device_id_type=MESH
        )

    def start(copy):
        copy.start()
        pending.append(copy)

    loads = [
        pltpu.make_async_copy(den, blk.at[c, 0], load_sem.at[0]),
        pltpu.make_async_copy(sus, blk.at[c, 1], load_sem.at[1]),
        pltpu.make_async_copy(cell, cell_v, load_sem.at[2]),
        pltpu.make_async_copy(line, line_v, load_sem.at[3]),
        pltpu.make_async_copy(obs, obs_v, load_sem.at[4]),
        pltpu.make_async_copy(wgt, wgt_v, load_sem.at[5]),
    ]
    for copy in loads:
        copy.start()
    barrier = pltpu.get_barrier_semaphore()
    partner = {"c": 1 - c}
    pl.semaphore_signal(barrier, inc=1, device_id=partner, device_id_type=MESH)
    for d in range(1, 8):
        q = (bx + d) % 8
        pl.semaphore_signal(barrier, inc=1, device_id={"xl": q // 4, "y": q % 4}, device_id_type=MESH)
        q = (by + d) % 8
        pl.semaphore_signal(barrier, inc=1, device_id={"xh": q // 4, "z": q % 4}, device_id_type=MESH)
    pl.semaphore_signal(barrier, inc=1, device_id={"xl": 1 - xl, "xh": 1 - xh}, device_id_type=MESH)

    for copy in loads:
        copy.wait()
    rows = []
    for ref in (cell_v, line_v, obs_v, wgt_v):
        value = ref[...].astype(f32)
        row = jnp.where(c == 0, value[0:1], value[1:2])
        rows += [row[:, :LANES], row[:, LANES:]]
    st[bx] = jnp.concatenate(rows, axis=0)
    big[...] = jnp.zeros_like(big)

    lane = iota((1, LANES), 1)
    dy = (NY - 1 - lane - j0).astype(f32)
    dx = (iota((US, 1), 0) - PAD - i0).astype(f32)
    rowv[...] = dx * dx + dy * dy

    def table_rows(tile, carry):
        depth = ((tile * 16 + iota((16, LANES), 0)).astype(f32) + 0.5) * cell_depth + lift
        square = depth * depth
        scale = jnp.where(c == 0, 0.0, 3.0 * square)
        shift = jnp.where(c == 0, depth, -1.0)
        first = pl.multiple_of(tile * 16, 16)
        for u in range(US):
            inverse = lax.rsqrt(square + rowv[u : u + 1, :])
            inv2 = inverse * inverse
            value = inv2 * inverse * (scale * inv2 + shift)
            high, low = split(value)
            tt[pl.ds(first, 16), u * LANES : (u + 1) * LANES] = high
            tt[pl.ds(first + NZ, 16), u * LANES : (u + 1) * LANES] = low
        return carry

    lax.fori_loop(0, 4, table_rows, 0)

    pl.semaphore_wait(barrier, 16)
    pair_blk = remote(blk.at[c], blk.at[c], pair_send.at[0], pair_recv.at[0], partner)
    start(pair_blk)
    for d in range(1, 8):
        q = (bx + d) % 8
        start(remote(st.at[bx], st.at[bx], st_send.at[d - 1], st_recv.at[bx], {"xl": q // 4, "y": q % 4}))

    lax.fori_loop(4, 8, table_rows, 0)

    pair_blk.wait_recv()
    qm = (bx + 7) % 8
    qp = (bx + 1) % 8
    left = {"xl": qm // 4, "y": qm % 4}
    right = {"xl": qp // 4, "y": qp % 4}
    halo_l = remote(blk.at[:, :, 0:2], xhi, halo_send.at[0], halo_recv.at[0], left)
    halo_r = remote(blk.at[:, :, 7:8], xlo, halo_send.at[1], halo_recv.at[1], right)
    start(halo_l)
    start(halo_r)

    def forward(columns):
        cells = jnp.concatenate([v.reshape(SIDE, 1, NZ) for v in columns], axis=1).reshape(SIDE * SIDE, NZ)
        high, low = split(cells)
        lhs = jnp.concatenate(
            [jnp.concatenate([high, high], axis=1), jnp.concatenate([low, jnp.zeros_like(low)], axis=1)], axis=0
        )
        sums = [None] * NX
        for t in range(US // 8):
            part = dot(lhs, tt[:, t * 8 * LANES : (t + 1) * 8 * LANES])
            part = part[: SIDE * SIDE] + part[SIDE * SIDE :]
            for uu in range(8):
                for i in range(SIDE):
                    x = t * 8 + uu - PAD + i
                    if 0 <= x < NX:
                        piece = part[i * SIDE : (i + 1) * SIDE, uu * LANES : (uu + 1) * LANES]
                        sums[x] = piece if sums[x] is None else sums[x] + piece
        grid = []
        for x in range(NX):
            turned = pltpu.roll(sums[x], 121, 1, stride=1, stride_axis=0)
            grid.append(jnp.sum(turned, axis=0, keepdims=True))
        upper = jnp.concatenate(grid[: NX // 2], axis=0)
        lower = jnp.concatenate(grid[NX // 2 :], axis=0)
        return jnp.where(lane < NY, upper, pltpu.roll(lower, NY, 1))

    def line_copies(buf, sends, recvs, stage):
        me = (px, y, z)[stage]
        copies = []
        for d in range(1, 4):
            q = (me + d) % 4
            device = ({"xh": q // 2, "xl": q % 2}, {"y": q}, {"z": q})[stage]
            out = remote(buf.at[stage, me], buf.at[stage, me], sends.at[stage, d - 1], recvs.at[stage, me], device)
            into = remote(buf.at[stage, q], buf.at[stage, q], sends.at[stage, d - 1], recvs.at[stage, q], device)
            copies.append((out, into))
        return me, copies

    def line_start(buf, sends, recvs, stage, value):
        me, copies = line_copies(buf, sends, recvs, stage)
        buf[stage, me] = value
        for out, _ in copies:
            start(out)
        return copies

    def line_wait(copies):
        for _, into in copies:
            into.wait_recv()

    def line_sum(buf, stage):
        return (buf[stage, 0] + buf[stage, 1]) + (buf[stage, 2] + buf[stage, 3])

    halves = [blk[core, c] for core in range(2)]
    columns = [halves[q // 4][:, q % 4, :] for q in reversed(range(SIDE))]
    first = line_start(ar1, a1_send, a1_recv, 0, forward(columns))

    for d in range(1, 8):
        q = (bx + d) % 8
        remote(st.at[q], st.at[q], st_send.at[d - 1], st_recv.at[q], partner).wait_recv()

    def station_row(index):
        return jnp.concatenate(
            [st[g, 2 * index + h : 2 * index + h + 1, :] for g in range(8) for h in range(2)], axis=1
        )

    station = station_row(0).astype(jnp.int32)
    station_x = station // NY
    station_m = NY - 1 - station % NY
    labels = station_row(1).astype(jnp.int32)
    label_h = labels // LANES
    label_l = labels % LANES
    data = station_row(2)
    weight = station_row(3)
    one = lambda mask: jnp.where(mask, 1.0, 0.0).astype(bf16)
    ohy[...] = one(iota((LANES, STATIONS), 0) == station_m)
    ohl[...] = one(iota((LANES, STATIONS), 0) == label_l)
    hmask = iota((8, STATIONS), 0) == label_h
    xmask = iota((NX, STATIONS), 0) == station_x
    hot = jnp.where(hmask, 1.0, 0.0)
    counts = dot_nt(jnp.concatenate([hot, jnp.zeros_like(hot)], axis=0).astype(bf16), ohl[...])[:8]
    inv_cnt[...] = 1.0 / jnp.maximum(counts, 1.0)

    line_wait(first)
    second = line_start(ar1, a1_send, a1_recv, 1, line_sum(ar1, 0))

    halo_l.wait_recv()
    halo_r.wait_recv()
    for f in range(2):
        for core in range(2):
            at = slice(1 + 4 * core, 5 + 4 * core)
            big[f, 1:9, at, :] = blk[core, f]
            big[f, 0:1, at, :] = xlo[core, f]
            big[f, 9:11, at, :] = xhi[core, f]
    ylo_s[...] = big[:, :, 1:3, :]
    yhi_s[...] = big[:, :, 8:9, :]
    qm = (by + 7) % 8
    qp = (by + 1) % 8
    halo_d = remote(ylo_s, yhi, halo_send.at[2], halo_recv.at[2], {"xh": qm // 4, "z": qm % 4})
    halo_u = remote(yhi_s, ylo, halo_send.at[3], halo_recv.at[3], {"xh": qp // 4, "z": qp % 4})
    start(halo_d)
    start(halo_u)

    line_wait(second)
    third = line_start(ar1, a1_send, a1_recv, 2, line_sum(ar1, 1))

    halo_d.wait_recv()
    halo_u.wait_recv()
    big[:, :, 9:11, :] = yhi[...]
    big[:, :, 0:1, :] = ylo[...]

    ni, nj = SIDE + 2, 16
    deep = iota((1, 1, NZ), 2) < NZ - 1
    gi = i0 - 1 + iota((ni, nj, NZ), 0)
    gj = j0 - 1 + iota((ni, nj, NZ), 1)
    along_i = gi < NX - 1
    along_j = gj < NY - 1
    valid = (gi >= 0) & (gj >= 0)

    def roll_j(value, shift):
        n = value.shape[0]
        return pltpu.roll(value, shift, 1)

    def roll_k(value, shift):
        return pltpu.roll(value, shift, 2)

    def diffs(value, mask_i, mask_j):
        base = value[:-1]
        return (
            jnp.where(mask_i, value[1:] - base, 0.0),
            jnp.where(mask_j, roll_j(base, nj - 1) - base, 0.0),
            jnp.where(deep, roll_k(base, NZ - 1) - base, 0.0),
        )

    def cross(a, b):
        return (a[1] * b[2] - a[2] * b[1], a[2] * b[0] - a[0] * b[2], a[0] * b[1] - a[1] * b[0])

    def inner(a, b):
        return a[0] * b[0] + a[1] * b[1] + a[2] * b[2]

    a = diffs(big[0], along_i, along_j)
    b = diffs(big[1], along_i, along_j)
    t = tuple(jnp.where(valid, v, 0.0) for v in cross(a, b))
    for f, pull in enumerate((cross(b, t), cross(t, a))):
        px_ = jnp.where(along_i, pull[0], 0.0)
        py_ = jnp.where(along_j, pull[1], 0.0)
        pz_ = jnp.where(deep, pull[2], 0.0)
        force = px_[:-1] - px_[1:]
        force = force + (roll_j(py_, 1) - py_)[1:]
        force = force + (jnp.where(iota((1, 1, NZ), 2) > 0, roll_k(pz_, 1), 0.0) - pz_)[1:]
        force = roll_j(force, nj - 1)
        cfb[f] = force
        cfo[f] = jnp.where(c == 0, force[:SIDE, 0:4], force[:SIDE, 4:8])
    out_cf = pltpu.make_async_copy(cfo, cf_out, out_sem.at[0])
    out_cf.start()

    line_wait(third)
    predicted = line_sum(ar1, 2)

    def gather(packed):
        both = jnp.concatenate([packed, pltpu.roll(packed, NY, 1)], axis=0)
        high, low = split(both)
        hit = dot(jnp.concatenate([high, low], axis=0), ohy[...])
        hit = hit[:NX] + hit[NX:]
        return jnp.sum(jnp.where(xmask, hit, 0.0), axis=0, keepdims=True)

    def masked_split(mask, value):
        high, low = rounded(value)
        return jnp.concatenate([jnp.where(mask, high, 0.0), jnp.where(mask, low, 0.0)], axis=0).astype(bf16)

    def level(value):
        sums = dot_nt(masked_split(hmask, value), ohl[...])
        means = (sums[:8] + sums[8:]) * inv_cnt[...]
        high, low = split(means)
        spread = dot(jnp.concatenate([high, low], axis=0), ohl[...])
        spread = spread[:8] + spread[8:]
        return value - jnp.sum(jnp.where(hmask, spread, 0.0), axis=0, keepdims=True)

    residual = level(gather(predicted) - data)
    weighted = weight * residual
    source = level(weight * weighted)

    hits = dot_nt(masked_split(xmask, source), ohy[...])
    sg = hits[:NX] + hits[NX:]
    zero = jnp.zeros((PAD, LANES), f32)
    parts = rounded(sg)
    for part, shifts, extra in zip(parts, (e_hi, e_lo), (x_hi, x_lo)):
        turned = [zero] * PAD
        for x in range(NX):
            row = jnp.broadcast_to(part[x : x + 1], (SIDE, LANES))
            turned.append(pltpu.roll(row, 0, 1, stride=1, stride_axis=0))
        turned += [zero] * (PAD + 2)
        for n in range(US + 8):
            shifts[:, n * LANES : (n + 1) * LANES] = jnp.concatenate([turned[n], turned[n + 1]], axis=0).astype(bf16)
        sgp[0:PAD] = zero
        sgp[PAD : PAD + NX] = pltpu.roll(part, SIDE, 1)
        sgp[PAD + NX : PAD + NX + 16] = jnp.zeros((16, LANES), f32)
        for u in range(US):
            extra[:, u * LANES : (u + 1) * LANES] = sgp[u : u + 16].astype(bf16)

    acc = None
    for t in range(US // 2):
        lanes = [slice((2 * t + 2 * p) * LANES, (2 * t + 2 * p + 2) * LANES) for p in range(5)]
        lhs = jnp.concatenate(
            [e_hi[:, s] for s in lanes] + [x_hi[:, lanes[0]]] + [e_lo[:, s] for s in lanes] + [x_lo[:, lanes[0]]],
            axis=0,
        )
        term = dot_nt(lhs, tt[:, lanes[0]])
        acc = term if acc is None else acc + term
    dg = acc[:96, :NZ] + acc[:96, NZ:] + acc[96:, :NZ]
    main = dg[:80].reshape(10, SIDE, NZ)
    dgb[c, :, 0:SIDE, :] = main
    for i in range(SIDE + 1):
        dgb[c, i, SIDE : SIDE + 1, :] = dg[80 + i : 81 + i]
    pair_dg = remote(dgb.at[c], dgb.at[c], pair_send.at[1], pair_recv.at[1], partner)
    start(pair_dg)

    own = main[:SIDE] + coupling * cfb[c, 0:SIDE, 0:SIDE, :]
    columns = [own[:, q, :] for q in reversed(range(SIDE))]
    first = line_start(ar2, a2_send, a2_recv, 0, forward(columns))

    for g in range(8):
        for h in range(2):
            at = (2 * g + h) * LANES
            wr_all[g, h : h + 1, :] = weighted[:, at : at + LANES]
    wrx[c] = wr_all[bx]
    pair_wr = remote(wrx.at[c], wrx.at[c], pair_send.at[2], pair_recv.at[2], partner)
    start(pair_wr)

    pair_dg.wait_recv()
    for f in range(2):
        dgo[f] = jnp.where(c == 0, dgb[f, 0:SIDE, 0:4, :], dgb[f, 0:SIDE, 4:8, :])
    out_dg = pltpu.make_async_copy(dgo, dg_out, out_sem.at[1])
    out_dg.start()

    grads = [dgb[f, 0 : SIDE + 1] + coupling * cfb[f] for f in range(2)]
    edge_i = i0 + iota((SIDE, nj, NZ), 0) < NX - 1
    edge_j = j0 + iota((SIDE, nj, NZ), 1) < NY - 1
    models = [roll_j(big[f, 1:10], nj - 1) for f in range(2)]

    def short(value):
        return tuple(v[:, 0:SIDE] for v in diffs(value, edge_i, edge_j))

    am, bm, ag, bg = (short(v) for v in (*models, *grads))
    t0 = cross(am, bm)
    t1 = tuple(p + q for p, q in zip(cross(ag, bm), cross(am, bg)))
    t2 = cross(ag, bg)
    energy = (
        inner(t0, t0),
        -2.0 * inner(t0, t1),
        inner(t1, t1) + 2.0 * inner(t0, t2),
        -2.0 * inner(t1, t2),
        inner(t2, t2),
    )
    terms = [jnp.sum(jnp.sum(e, axis=0), axis=0, keepdims=True) for e in energy]
    largest = jnp.maximum(jnp.abs(grads[0][:SIDE, 0:SIDE]), jnp.abs(grads[1][:SIDE, 0:SIDE]))
    terms.append(jnp.max(jnp.max(largest, axis=0), axis=0, keepdims=True))
    terms.append(jnp.zeros((2, LANES), f32))
    small = jnp.concatenate(terms, axis=0)
    is_peak = iota((8, LANES), 0) == 5

    def small_sum(stage):
        p, q, r, s = (ar3[stage, n] for n in range(4))
        top = jnp.maximum(jnp.maximum(p, q), jnp.maximum(r, s))
        return jnp.where(is_peak, top, (p + q) + (r + s))

    line_wait(first)
    second = line_start(ar2, a2_send, a2_recv, 1, line_sum(ar2, 0))
    small_1 = line_start(ar3, a3_send, a3_recv, 0, small)
    pair_wr.wait_recv()
    for f in range(2):
        for h in range(2):
            wro[f : f + 1, h * LANES : (h + 1) * LANES] = wrx[f, h : h + 1, :]
    out_wr = pltpu.make_async_copy(wro, wr_out, out_sem.at[2])
    out_wr.start()
    line_wait(second)
    third = line_start(ar2, a2_send, a2_recv, 2, line_sum(ar2, 1))
    line_wait(small_1)
    small_2 = line_start(ar3, a3_send, a3_recv, 1, small_sum(0))
    line_wait(third)
    image = line_sum(ar2, 2)
    line_wait(small_2)
    small_3 = line_start(ar3, a3_send, a3_recv, 2, small_sum(1))
    change = level(gather(image))
    line_wait(small_3)
    small = small_sum(2)

    peak = jnp.max(small, axis=1, keepdims=True)[5:6] + 1e-06
    totals = jnp.sum(small, axis=1, keepdims=True)
    tau = jnp.zeros((TRIALS, LANES), f32)
    for k in range(TRIALS):
        tau = jnp.where(iota((TRIALS, LANES), 0) == k, steps[k], tau)
    tau = tau / peak
    moved = weight * (residual - tau[:, 0:1] * change)
    value = 0.5 * jnp.sum(moved * moved, axis=1, keepdims=True)
    fin[c] = jnp.broadcast_to(value, (TRIALS, LANES))
    pair_fin = remote(fin.at[c], fin.at[c], pair_send.at[3], pair_recv.at[3], partner)
    start(pair_fin)
    poly = totals[4:5]
    for n in (3, 2, 1, 0):
        poly = poly * tau + totals[n : n + 1]
    pair_fin.wait_recv()
    tvo[...] = ((fin[0] + fin[1]) + coupling * 0.5 * poly) / (2.0 * STATIONS)
    out_tv = pltpu.make_async_copy(tvo, tv_out, out_sem.at[3])
    out_tv.start()
    for copy in pending:
        copy.wait_send()
    for copy in (out_cf, out_dg, out_wr, out_tv):
        copy.wait()


def body(density, susceptibility, station_cell, station_line, observed, data_weight, trial_steps):
    hbm = pl.BlockSpec(memory_space=pl.ANY)
    vmem = lambda *shape: pltpu.VMEM(shape, f32)
    half = lambda *shape: pltpu.VMEM(shape, bf16)
    sem = lambda *shape: pltpu.SemaphoreType.DMA(shape)
    scratch = [
        vmem(2, 2, SIDE, 4, NZ),
        pltpu.VMEM((2, 256), jnp.int32), pltpu.VMEM((2, 256), jnp.int32), vmem(2, 256), vmem(2, 256),
        vmem(8, 8, LANES),
        vmem(US, LANES),
        half(2 * NZ, US * LANES),
        vmem(3, 4, NX // 2, LANES), vmem(3, 4, NX // 2, LANES), vmem(3, 4, 8, LANES),
        half(NX, STATIONS), half(LANES, STATIONS), half(LANES, STATIONS),
        vmem(2, 2, 1, 4, NZ), vmem(2, 2, 2, 4, NZ),
        vmem(2, 11, 2, NZ), vmem(2, 11, 1, NZ), vmem(2, 11, 1, NZ), vmem(2, 11, 2, NZ),
        vmem(2, 11, 16, NZ),
        half(16, (US + 8) * LANES), half(16, (US + 8) * LANES), half(16, US * LANES), half(16, US * LANES),
        vmem(PAD + NX + 16, LANES),
        vmem(2, 10, 16, NZ), vmem(2, SIDE + 1, 16, NZ),
        vmem(2, SIDE, 4, NZ), vmem(2, SIDE, 4, NZ),
        vmem(8, 2, LANES), vmem(2, 2, LANES), vmem(2, 256), vmem(2, TRIALS, LANES), vmem(TRIALS, LANES),
        vmem(8, LANES),
        sem(6), sem(4), sem(4), sem(4), sem(7), sem(8),
        sem(3, 3), sem(3, 4), sem(3, 3), sem(3, 4), sem(3, 3), sem(3, 4), sem(4), sem(4),
    ]
    shape = lambda *s: jax.ShapeDtypeStruct(s, f32)
    dg, cf, wr, tv = pl.pallas_call(
        kernel,
        out_shape=(shape(2, SIDE, 4, NZ), shape(2, SIDE, 4, NZ), shape(2, 256), shape(TRIALS, LANES)),
        in_specs=[hbm] * 6 + [pl.BlockSpec(memory_space=pltpu.SMEM)],
        out_specs=(hbm,) * 4,
        scratch_shapes=scratch,
        compiler_params=pltpu.CompilerParams(
            collective_id=0, has_side_effects=True, vmem_limit_bytes=48 * 1024 * 1024
        ),
    )(density, susceptibility, station_cell, station_line, observed, data_weight, trial_steps)
    return dg, cf, wr, tv[:, 0]


def solution(mesh):
    torus = Mesh(mesh.devices.reshape(2, 4, 2, 4, 2), AXES)
    in_specs = (
        P(GX, GY, None), P(GX, GY, None), P(None, GX), P(None, GX), P(None, GX), P(None, GX), P(),
    )
    out_specs = (P(None, GX, GY, None), P(None, GX, GY, None), P(None, GX), P())
    return jax.shard_map(body, mesh=torus, in_specs=in_specs, out_specs=out_specs, check_vma=False)
```
